768 devices in a mesh: owner: 16 (over z_hi, x, core), shard: 48 (over y, z_lo).
Axes of the slice: x: 4, y: 8, z: 12 (z_hi: 2, z_lo: 6; z = z_hi * 6 + z_lo), core: 2. Of those that a mesh axis runs over, the one named last changes fastest.
Arguments:
- tokens: bfloat16 [576, 7168], P('shard', 'owner'), may hold values from -6 to 6
- expert_ids: int32 [576, 8], P('shard'), may hold values from 0 to 47, all different within a row; in each aligned block of 12 rows (0 to 11, 12 to 23, ...) at most 3 rows name the same one
- gate_weight: bfloat16 [48, 7168, 1024], P('shard', 'owner'), may hold values from -0.0625 to 0.0625
- up_weight: bfloat16 [48, 7168, 1024], P('shard', 'owner'), may hold values from -0.0625 to 0.0625
- trainer_down: float32 [48, 1024, 7168], P('shard', None, 'owner'), may hold values from -0.1875 to 0.1875
Outputs:
- hidden: bfloat16 [144, 48, 1024], P('owner', 'shard')
- new_down: bfloat16 [48, 1024, 7168], P('shard', 'owner')
The draws below stay inside these ranges and needn't reach their ends.
Inputs may be any that keep to these rules, and one draw needn't show every extreme that they name: `expert_ids`: within the rows of one index of shard (aligned blocks of 12 rows) no expert is named by more than 3 rows, a bound that some block reaches.
All inputs are finite; a program needn't handle non-finite values.
Results may differ from the reference program's by a relative error of at most 0.0017.
Values may be sent and summed in bfloat16 or wider, within the bound.
No kernel may reach another device: no remote copies, remote signals or barrier semaphores. Data moves between devices by JAX's collectives and lax.ppermute only.
A program may use at most 32 MiB of HBM per device.

```python
import math
import jax
import jax.numpy as jnp
import numpy as np
from jax import lax

D = 7168
TOP = 8
FF = 1024
EXPERTS = 48
ROWS_DEV = 12
CAP = 3
ROWS = 576
N_SHARD = 48


def shard_levels(stream_key, shape, pieces, least, top_value):
    def one(position, parts):
        steps = jax.random.uniform(jax.random.fold_in(jax.random.fold_in(stream_key, 6), position), (parts,), jnp.float32, least / len(pieces), top_value / len(pieces))
        return jnp.repeat(jnp.exp(steps), shape[position] // parts).reshape((-1,) + (1,) * (len(shape) - position - 1))

    factor_of = one(*pieces[0])
    for cut in pieces[1:]:
        factor_of = factor_of * one(*cut)
    return factor_of


def routed_block(own_key, own, number, rows, number_of, top, reach, slope):
    ranking = jax.random.permutation(own_key, number_of)
    heavy_load, ordinary = load_shares(number_of, rows * top, reach, slope, True), load_shares(number_of, rows * top, reach, slope, False)
    places = jnp.arange(number_of)

    def named(tallies, rotation):
        used = int((tallies > 0).sum())
        fixed = max(1, used // 4)
        moved = fixed + (places - fixed + rotation * (used - fixed)) % max(1, number_of - fixed)
        return jnp.zeros((number_of,), jnp.int32).at[ranking[jnp.where(places < fixed, places, moved)]].set(jnp.asarray(tallies, jnp.int32))

    tallies = jnp.where(number % 4 == 0, named(heavy_load, number // 4), named(ordinary, number - number // 4 - 1))
    mixed = jax.random.permutation(jax.random.fold_in(own, 3), number_of)
    donor, taker = mixed[0:number_of // 2 * 2:2], mixed[1:number_of // 2 * 2:2]
    slack = jnp.minimum(tallies[donor] - 1, reach - tallies[taker]) // 2
    slack = jnp.where((donor == ranking[0]) | (taker == ranking[0]) | (tallies[taker] == 0), 0, jnp.maximum(slack, 0))
    moved = jax.random.randint(jax.random.fold_in(own, 4), (number_of // 2,), 0, 1 << 20) % (slack + 1)
    tallies = tallies.at[donor].add(-moved).at[taker].add(moved)
    labels = jnp.searchsorted(jnp.cumsum(tallies), jnp.arange(rows * top), side="right").astype(jnp.int32)
    grid = labels.reshape(top, rows).T
    grid = grid[jax.random.permutation(jax.random.fold_in(own, 1), rows)]
    rotation = jax.random.randint(jax.random.fold_in(own, 2), (rows, 1), 0, top)
    return jnp.take_along_axis(grid, (jnp.arange(top)[None, :] + rotation) % top, axis=1)


def load_shares(count, total, reach, slope, full):
    loads = [(1 << 20) // math.isqrt(rank ** slope) + 1 for rank in range(1, count + 1)]
    largest = reach if full else min(reach, max(-(-total // count), total * loads[0] // sum(loads)))
    least = 1 if total - largest >= count - 1 else 0
    given, spare = [largest] + [least] * (count - 1), total - largest - least * (count - 1)
    while spare > 0:
        free = [i for i in range(1, count) if given[i] < largest] or [i for i in range(1, count) if given[i] < reach]
        mass, remaining = sum([loads[i] for i in free]), spare
        for i in free:
            addition = min(reach - given[i], max(1, remaining * loads[i] // mass), spare)
            given[i] = given[i] + addition
            spare = spare - addition
    return np.array(given)


def centred(stream_key, extent, spread, reach, pieces=(), kind=jnp.bfloat16):
    entries = spread * jax.random.normal(stream_key, extent, jnp.float32)
    if pieces:
        entries = entries * shard_levels(stream_key, extent, pieces, -0.22, 0.18)
    return jnp.clip(entries, -reach, reach).astype(kind)


def setup_inputs(seed: int = 0) -> dict:
    arg_keys = jax.random.split(jax.random.key(seed), 6)
    tokens = centred(arg_keys[0], (ROWS, D), 1.0, 6.0, ((0, 48), (1, 16)))
    expert_ids_keys = jax.random.split(jax.random.fold_in(arg_keys[1], 1), ROWS // ROWS_DEV)
    expert_ids_turns = jax.random.permutation(jax.random.fold_in(arg_keys[1], 3), ROWS // ROWS_DEV)
    expert_ids = jax.vmap(lambda own, number: routed_block(jax.random.fold_in(arg_keys[1], 2), own, number, ROWS_DEV, EXPERTS, TOP, CAP, 2))(expert_ids_keys, expert_ids_turns).reshape((ROWS, TOP))
    gate_weight = centred(arg_keys[2], (EXPERTS, D, FF), D ** -0.5, 0.0625, ((0, 48), (1, 16)))
    up_weight = centred(arg_keys[3], (EXPERTS, D, FF), D ** -0.5, 0.0625, ((0, 48), (1, 16)))
    trainer_down = centred(arg_keys[4], (EXPERTS, FF, D), FF ** -0.5, 0.1875, ((0, 48), (2, 16)), jnp.float32)
    return dict(tokens=tokens, expert_ids=expert_ids, gate_weight=gate_weight, up_weight=up_weight, trainer_down=trainer_down)


def place_block(block):
    block_tokens, block_ids = block
    flat = block_ids.reshape(-1)
    hits = (flat[:, None] == jnp.arange(EXPERTS, dtype=jnp.int32)[None, :]).astype(jnp.int32)
    before = jnp.cumsum(hits, axis=0) - hits
    place = jnp.sum(before * hits, axis=1)
    target = place * EXPERTS + flat
    select = (target[:, None] == jnp.arange(CAP * EXPERTS, dtype=jnp.int32)[None, :]).astype(jnp.int32)
    select = jnp.sum(select.reshape(ROWS_DEV, TOP, CAP * EXPERTS), axis=1).astype(block_tokens.dtype)
    sent = jnp.dot(select.T, block_tokens, preferred_element_type=jnp.float32)
    return sent.astype(jnp.bfloat16).reshape(CAP, EXPERTS, D)


def reference(tokens, expert_ids, gate_weight, up_weight, trainer_down):
    token_blocks = tokens.reshape(N_SHARD, ROWS_DEV, D)
    id_blocks = expert_ids.reshape(N_SHARD, ROWS_DEV, TOP)
    sends = lax.map(place_block, (token_blocks, id_blocks))
    dispatched = sends.reshape(N_SHARD * CAP, EXPERTS, D)
    by_expert = jnp.swapaxes(dispatched, 0, 1)

    def one_expert(item):
        rows, gate_one, up_one = item
        gate = jnp.dot(rows, gate_one, preferred_element_type=jnp.float32)
        up = jnp.dot(rows, up_one, preferred_element_type=jnp.float32)
        return (jax.nn.silu(gate) * up).astype(jnp.bfloat16)

    hidden = lax.map(one_expert, (by_expert, gate_weight, up_weight))
    hidden = jnp.swapaxes(hidden, 0, 1)
    new_down = trainer_down.astype(jnp.bfloat16)
    return hidden, new_down
```

```python
import jax
import jax.numpy as jnp
from jax import lax
from jax.experimental import pallas as pl
from jax.experimental.pallas import tpu as pltpu
from jax.sharding import PartitionSpec as P

FF = 1024
EXPERTS = 48
NX = 4
NY = 8
NZ = 6
LANES = 128
BF16 = jnp.bfloat16
F32 = jnp.float32

OCTET = [list(range(8)), list(range(8, 16))]
ALONG_X = [[h * 8 + x * 2 + c for x in range(NX)] for h in range(2) for c in range(2)]
SWAP_CORE = [(o, o ^ 1) for o in range(16)]
SWAP_HALF = [(o, o ^ 8) for o in range(16)]


def iota(shape, dim):
    return lax.broadcasted_iota(jnp.int32, shape, dim)


def vmem():
    return pl.BlockSpec(memory_space=pltpu.VMEM)


def smem():
    return pl.BlockSpec(memory_space=pltpu.SMEM)


def pack_kernel(ids_ref, tokens_ref, out_ref):
    n = EXPERTS * 16
    rows = tokens_ref.shape[0]
    width = tokens_ref.shape[1]
    ids = ids_ref[...]
    line = iota((n, rows), 0)
    expert = line >> 4
    hit = jnp.zeros((n, rows), jnp.bool_)
    for k in range(ids.shape[0]):
        hit = hit | (ids[k : k + 1, :] == expert)
    earlier = jnp.where(iota((rows, rows), 0) < iota((rows, rows), 1), 1.0, 0.0).astype(BF16)
    hits = jnp.where(hit, 1.0, 0.0)
    before = jnp.dot(hits.astype(BF16), earlier, preferred_element_type=F32)
    slot = ((line >> 2) & 3).astype(F32)
    taken = jnp.where(before == slot, hits, 0.0)
    total = jnp.zeros((n, LANES), F32)
    for b in range(4):
        part = tokens_ref[:, b * LANES : min((b + 1) * LANES, width)]
        if part.shape[1] < LANES:
            part = jnp.concatenate([part, jnp.zeros((rows, LANES - part.shape[1]), BF16)], axis=1)
        pick = jnp.where((line & 3) == b, taken, 0.0).astype(BF16)
        total = total + jnp.dot(pick, part, preferred_element_type=F32)
    out_ref[...] = total.astype(BF16)


def project_kernel(core_ref, got_ref, gate_ref, up_ref, keep_ref, send_ref):
    core = core_ref[0]
    n = EXPERTS * 16
    m = 144
    width = gate_ref.shape[0]
    line = iota((m, n), 0)
    other = jnp.where(line >= 72, 1, 0)
    line = line - other * 72
    last = jnp.where(line >= 64, 1, 0)
    xh = jnp.where(last == 1, line - 64, line >> 3)
    s = jnp.where(last == 1, 8, line & 7)
    owner = (xh & 1) * 8 + (xh >> 1) * 2 + (core ^ other)
    slot = owner * 9 + s
    block = (slot * 171) >> 9
    source = block * 16 + (slot - block * 3) * 4
    column = iota((m, n), 1)
    got = got_ref[...]
    parts = []
    for b in range(4):
        pick = jnp.where(column == source + b, 1.0, 0.0).astype(BF16)
        part = jnp.dot(pick, got, preferred_element_type=F32).astype(BF16)
        if (b + 1) * LANES > width:
            part = part[:, : width - b * LANES]
        parts.append(part)
    rows = jnp.concatenate(parts, axis=1)
    gate = jnp.dot(rows, gate_ref[...], preferred_element_type=F32)
    up = jnp.dot(rows, up_ref[...], preferred_element_type=F32)
    for p, out_ref in enumerate((keep_ref, send_ref)):
        for q in range(8):
            x, h = q // 2, q % 2
            for j in range(16):
                src = gate if j < 8 else up
                lane = (j % 8) * LANES
                at = p * 72 + q * 8
                out_ref[x, h * 144 + j * 8 : h * 144 + j * 8 + 8, :] = src[at : at + 8, lane : lane + LANES]
                at = p * 72 + 64 + q
                out_ref[x, h * 144 + 128 + j : h * 144 + 129 + j, :] = src[at : at + 1, lane : lane + LANES]


def hidden_kernel(a_ref, b_ref, out_ref):
    total = a_ref[...] + b_ref[...]

    def gated(v, u):
        return v / (1.0 + jnp.exp(-v)) * u

    tail = gated(total[128:136], total[136:144])
    for j in range(8):
        head = gated(total[j * 8 : j * 8 + 8], total[64 + j * 8 : 72 + j * 8])
        both = jnp.concatenate([head, jnp.broadcast_to(tail[j : j + 1], (8, LANES))], axis=0)
        out_ref[:, j * LANES : (j + 1) * LANES] = both.astype(BF16)[:9]


def split_kernel(down_ref, out_ref):
    low = iota((down_ref.shape[0], LANES), 1) < 64
    for k in range(4):
        a = down_ref[:, k * LANES : (k + 1) * LANES]
        b = down_ref[:, (k + 4) * LANES : (k + 5) * LANES]
        out_ref[2 * k] = jnp.where(low, a, pltpu.roll(b, 64, 1)).astype(BF16)
        out_ref[2 * k + 1] = jnp.where(low, pltpu.roll(a, 64, 1), b).astype(BF16)


def turn_kernel(half_ref, in_ref, keep_ref, send_ref):
    half = half_ref[0]
    shape = (LANES, LANES)
    eye = jnp.where((iota(shape, 0) ^ (half * 64)) == iota(shape, 1), 1.0, 0.0).astype(BF16)
    turned = lax.dot_general(eye, in_ref[...], (((1,), (1,)), ((), ())), preferred_element_type=F32)
    turned = turned.astype(BF16)
    keep_ref[...] = turned[:64]
    send_ref[...] = turned[64:]


def join_kernel(half_ref, keep_ref, got_ref, out_ref):
    half = half_ref[0]
    width = keep_ref.shape[1]
    out_ref[:, pl.ds(pl.multiple_of(half * width, LANES), width)] = keep_ref[...]
    out_ref[:, pl.ds(pl.multiple_of((1 - half) * width, LANES), width)] = got_ref[...]


def on_device(tokens, expert_ids, gate_weight, up_weight, trainer_down):
    rows, width = tokens.shape
    owner = lax.axis_index("owner")
    half = (owner // 8).astype(jnp.int32).reshape(1)
    core = (owner % 2).astype(jnp.int32).reshape(1)

    packed = pl.pallas_call(
        pack_kernel,
        out_shape=jax.ShapeDtypeStruct((EXPERTS * 16, LANES), BF16),
        in_specs=[vmem(), vmem()],
        out_specs=vmem(),
        name="pack",
    )(expert_ids.T, tokens)
    with jax.named_scope("dispatch"):
        got = lax.all_to_all(
            packed.reshape(EXPERTS, 16, LANES), "shard", split_axis=0, concat_axis=0, tiled=True
        )

    down = jnp.swapaxes(trainer_down, 1, 2).reshape(width, 1024)
    pieces = pl.pallas_call(
        split_kernel,
        grid=(4,),
        out_shape=jax.ShapeDtypeStruct((8, width, LANES), BF16),
        in_specs=[pl.BlockSpec((width // 4, 1024), lambda i: (i, 0))],
        out_specs=pl.BlockSpec((8, width // 4, LANES), lambda i: (0, i, 0)),
        name="split",
    )(down)
    with jax.named_scope("downx"):
        columns = lax.all_to_all(
            pieces, "owner", split_axis=0, concat_axis=0, tiled=True, axis_index_groups=OCTET
        )
    wide = 8 * width
    step = wide // 7
    down_keep, down_send = pl.pallas_call(
        turn_kernel,
        grid=(7,),
        out_shape=[jax.ShapeDtypeStruct((64, wide), BF16)] * 2,
        in_specs=[smem(), pl.BlockSpec((step, LANES), lambda i: (i, 0))],
        out_specs=[pl.BlockSpec((64, step), lambda i: (0, i))] * 2,
        name="turn",
    )(half, columns.reshape(wide, LANES))
    with jax.named_scope("downz"):
        down_got = lax.ppermute(down_send, "owner", SWAP_HALF)

    keep, send = pl.pallas_call(
        project_kernel,
        out_shape=[jax.ShapeDtypeStruct((NX, 288, LANES), F32)] * 2,
        in_specs=[smem()] + [vmem()] * 3,
        out_specs=[vmem()] * 2,
        name="project",
    )(core, got.reshape(EXPERTS * 16, LANES), gate_weight[0], up_weight[0])
    with jax.named_scope("sumc"):
        pair = keep + lax.ppermute(send, "owner", SWAP_CORE)
    with jax.named_scope("sumx"):
        summed = lax.all_to_all(
            pair, "owner", split_axis=0, concat_axis=0, tiled=True, axis_index_groups=ALONG_X
        ).sum(axis=0)
    summed = summed.reshape(2, 144, LANES)
    mine = lax.dynamic_index_in_dim(summed, half[0], 0, keepdims=False)
    theirs = lax.dynamic_index_in_dim(summed, 1 - half[0], 0, keepdims=False)
    with jax.named_scope("sumz"):
        added = lax.ppermute(theirs, "owner", SWAP_HALF)
    hidden = pl.pallas_call(
        hidden_kernel,
        out_shape=jax.ShapeDtypeStruct((9, FF), BF16),
        in_specs=[vmem()] * 2,
        out_specs=vmem(),
        name="hidden",
    )(mine, added)

    new_down = pl.pallas_call(
        join_kernel,
        out_shape=jax.ShapeDtypeStruct((64, 2 * wide), BF16),
        in_specs=[smem()] + [vmem()] * 2,
        out_specs=vmem(),
        name="join",
    )(half, down_keep, down_got)
    return hidden.reshape(9, 1, FF), new_down.reshape(1, 64, 2 * wide)


def solution(mesh):
    in_specs = (
        P("shard", "owner"),
        P("shard", None),
        P("shard", "owner", None),
        P("shard", "owner", None),
        P("shard", None, "owner"),
    )
    out_specs = (P("owner", "shard", None), P("shard", "owner", None))
    return jax.shard_map(
        on_device, mesh=mesh, in_specs=in_specs, out_specs=out_specs, check_vma=False
    )
```

```python
import jax
import jax.numpy as jnp
from jax import lax
from jax.experimental import pallas as pl
from jax.experimental.pallas import tpu as pltpu
from jax.sharding import PartitionSpec as P


FF = 1024
EXPERTS = 48
NX = 4
LANES = 128
BF16 = jnp.bfloat16
F32 = jnp.float32

OCTET = [list(range(8)), list(range(8, 16))]
ALONG_X = [[(o, o & 9 | (o + 2 * d) & 6) for o in range(16)] for d in range(NX)]
SWAP_CORE = [(o, o ^ 1) for o in range(16)]
SWAP_HALF = [(o, o ^ 8) for o in range(16)]


def iota(shape, dim):
    return lax.broadcasted_iota(jnp.int32, shape, dim)


def vmem():
    return pl.BlockSpec(memory_space=pltpu.VMEM)


def smem():
    return pl.BlockSpec(memory_space=pltpu.SMEM)


def packed(ids_ref, tokens_ref):
    n = EXPERTS * 16
    rows = tokens_ref.shape[0]
    width = tokens_ref.shape[1]
    ids = ids_ref[...]
    line = iota((n, rows), 0)
    expert = line >> 4
    hit = jnp.zeros((n, rows), jnp.bool_)
    for k in range(ids.shape[0]):
        hit = hit | (ids[k : k + 1, :] == expert)
    earlier = jnp.where(iota((rows, rows), 0) < iota((rows, rows), 1), 1.0, 0.0).astype(BF16)
    hits = jnp.where(hit, 1.0, 0.0)
    before = jnp.dot(hits.astype(BF16), earlier, preferred_element_type=F32)
    slot = ((line >> 2) & 3).astype(F32)
    taken = jnp.where(before == slot, hits, 0.0)
    total = jnp.zeros((n, LANES), F32)
    for b in range(4):
        part = tokens_ref[:, b * LANES : min((b + 1) * LANES, width)]
        if part.shape[1] < LANES:
            part = jnp.concatenate([part, jnp.zeros((rows, LANES - part.shape[1]), BF16)], axis=1)
        pick = jnp.where((line & 3) == b, taken, 0.0).astype(BF16)
        total = total + jnp.dot(pick, part, preferred_element_type=F32)
    return total.astype(BF16)


def project_kernel(core_ref, got_ref, gate_ref, up_ref, keep_ref, send_ref):
    core = core_ref[0]
    n = EXPERTS * 16
    m = 144
    width = gate_ref.shape[0]
    line = iota((m, n), 0)
    other = jnp.where(line >= 72, 1, 0)
    line = line - other * 72
    last = jnp.where(line >= 64, 1, 0)
    xh = jnp.where(last == 1, line - 64, line >> 3)
    s = jnp.where(last == 1, 8, line & 7)
    owner = (xh & 1) * 8 + (xh >> 1) * 2 + (core ^ other)
    slot = owner * 9 + s
    block = (slot * 171) >> 9
    source = block * 16 + (slot - block * 3) * 4
    column = iota((m, n), 1)
    got = got_ref[...]
    parts = []
    for b in range(4):
        pick = jnp.where(column == source + b, 1.0, 0.0).astype(BF16)
        part = jnp.dot(pick, got, preferred_element_type=F32).astype(BF16)
        if (b + 1) * LANES > width:
            part = part[:, : width - b * LANES]
        parts.append(part)
    rows = jnp.concatenate(parts, axis=1)
    gate = jnp.dot(rows, gate_ref[...], preferred_element_type=F32)
    up = jnp.dot(rows, up_ref[...], preferred_element_type=F32)
    for p, out_ref in enumerate((keep_ref, send_ref)):
        for q in range(8):
            x, h = q // 2, q % 2
            for j in range(16):
                src = gate if j < 8 else up
                lane = (j % 8) * LANES
                at = p * 72 + q * 8
                out_ref[x, h * 144 + j * 8 : h * 144 + j * 8 + 8, :] = src[at : at + 8, lane : lane + LANES]
                at = p * 72 + 64 + q
                out_ref[x, h * 144 + 128 + j : h * 144 + 129 + j, :] = src[at : at + 1, lane : lane + LANES]


def hidden_kernel(a_ref, b_ref, out_ref):
    total = a_ref[...] + b_ref[...]

    def gated(v, u):
        return v / (1.0 + jnp.exp(-v)) * u

    tail = gated(total[128:136], total[136:144])
    for j in range(8):
        head = gated(total[j * 8 : j * 8 + 8], total[64 + j * 8 : 72 + j * 8])
        both = jnp.concatenate([head, jnp.broadcast_to(tail[j : j + 1], (8, LANES))], axis=0)
        out_ref[:, j * LANES : (j + 1) * LANES] = both.astype(BF16)[:9]


def add_kernel(x_ref, a_ref, b_ref, *out_refs):
    for d, out_ref in enumerate(out_refs):
        at = (x_ref[0] + d) & 3
        out_ref[...] = a_ref[at] + b_ref[at]


def fold_kernel(half_ref, a_ref, b_ref, c_ref, d_ref, mine_ref, theirs_ref):
    half = half_ref[0]
    for at, out_ref in ((half, mine_ref), (1 - half, theirs_ref)):
        rows = pl.ds(pl.multiple_of(at * 144, 8), 144)
        out_ref[...] = (a_ref[rows] + b_ref[rows]) + (c_ref[rows] + d_ref[rows])


def quarters(parts):
    n = parts[0][0].shape[0]
    group = iota((n, LANES), 1) >> 5
    out = None
    for q, (tile, offset) in enumerate(parts):
        tile = tile.astype(F32)
        if offset != 32 * q:
            tile = pltpu.roll(tile, (32 * q - offset) % LANES, 1)
        out = tile if out is None else jnp.where(group == q, tile, out)
    return out.astype(BF16)


def prepare_kernel(half_ref, ids_ref, tokens_ref, down_ref, rows_ref, p_ref, down, rows, p, sems):
    lanes = pl.ds(pl.multiple_of((1 - half_ref[0]) * 512, LANES), 512)
    load = pltpu.make_async_copy(down_ref.at[:, lanes], down, sems.at[0])
    store_rows = pltpu.make_async_copy(rows, rows_ref, sems.at[1])
    store_p = pltpu.make_async_copy(p, p_ref, sems.at[2])
    load.start()
    rows[...] = packed(ids_ref, tokens_ref)
    store_rows.start()
    load.wait()
    for t in range(2):
        parts = []
        for j in range(4 * t, 4 * t + 4):
            k = j // 2 * LANES
            parts.append((down[:, k : k + LANES], j % 2 * 64))
        p[:, t * LANES : (t + 1) * LANES] = quarters(parts)
    store_p.start()
    store_rows.wait()
    store_p.wait()


def split_p_kernel(half_ref, down_ref, got_ref, out_ref):
    n = out_ref.shape[1]
    for j in range(8):
        k, g = j // 2 * LANES, j // 4 * LANES
        parts = []
        for w in range(2):
            rows = slice(w * n, (w + 1) * n)
            parts.append((down_ref[rows, k : k + LANES], j % 2 * 64))
            parts.append((got_ref[rows, g : g + LANES], j % 4 * 32))
        out_ref[j] = quarters(parts)


def split_q_kernel(down_ref, out_ref):
    n = out_ref.shape[1]
    for j in range(8):
        k = j // 2 * LANES
        parts = []
        for w in range(2):
            for h in range(2):
                at = h * 512 + k
                parts.append((down_ref[w * n : (w + 1) * n, at : at + LANES], j % 2 * 64 + 32))
        out_ref[j] = quarters(parts)


def load_kernel(gate_ref, up_ref, gate_out_ref, up_out_ref, sems):
    copies = [
        pltpu.make_async_copy(gate_ref, gate_out_ref, sems.at[0]),
        pltpu.make_async_copy(up_ref, up_out_ref, sems.at[1]),
    ]
    for copy in copies:
        copy.start()
    for copy in copies:
        copy.wait()


def turned(ref):
    n = ref.shape[1]
    low = iota((n, LANES), 1) < 64
    zero = jnp.zeros((n, LANES), BF16)
    parts = []
    for q in range(8):
        block = ref[q]
        parts += [jnp.where(low, block, zero), jnp.where(low, zero, block)]
    stack = jnp.concatenate(parts, axis=0)
    i, k = iota((64, LANES), 0), iota((64, LANES), 1)
    eye = jnp.where((i == k) | (i + 64 == k), 1.0, 0.0).astype(BF16)
    out = lax.dot_general(eye, stack, (((1,), (1,)), ((), ())), preferred_element_type=F32)
    return out.astype(BF16)


def turn_q_kernel(half_ref, in_ref, keep_ref, send_ref):
    rows = turned(in_ref)
    first = half_ref[0] == 0
    keep_ref[...] = jnp.where(first, rows[:32], rows[32:])
    send_ref[...] = jnp.where(first, rows[32:], rows[:32])


def join_kernel(half_ref, p_ref, keep_ref, got_ref, out_ref):
    width = keep_ref.shape[1]
    own = pl.ds(pl.multiple_of(half_ref[0] * width, LANES), width)
    other = pl.ds(pl.multiple_of((1 - half_ref[0]) * width, LANES), width)
    rows = turned(p_ref)
    out_ref[:32, own] = rows[:32]
    out_ref[:32, other] = rows[32:]
    out_ref[32:, own] = keep_ref[...]
    out_ref[32:, other] = got_ref[...]


def chip(x):
    return pltpu.with_memory_space_constraint(x, pltpu.VMEM)


def half_of_down(kernel, out, half, down, other, *more):
    width = down.shape[0]
    return pl.pallas_call(
        kernel,
        out_shape=jax.ShapeDtypeStruct(out, BF16),
        grid_spec=pltpu.PrefetchScalarGridSpec(
            num_scalar_prefetch=1,
            grid=(1,),
            in_specs=[pl.BlockSpec((width, 512), lambda i, h: (0, (1 - h[0]) if other else h[0]))]
            + [vmem() for _ in more],
            out_specs=vmem(),
        ),
    )(half, down, *more)


def over_x(x):
    return lax.all_to_all(
        x, "owner", split_axis=0, concat_axis=0, tiled=True, axis_index_groups=OCTET
    )


def on_device(tokens, expert_ids, gate_weight, up_weight, trainer_down):
    _, width = tokens.shape
    owner = lax.axis_index("owner")
    half = (owner >> 3).astype(jnp.int32).reshape(1)
    core = (owner & 1).astype(jnp.int32).reshape(1)
    place = ((owner >> 1) & 3).astype(jnp.int32).reshape(1)
    down = jnp.swapaxes(trainer_down, 1, 2).reshape(width, 1024)

    shapes = [(EXPERTS * 16, LANES), (width, 256)]
    anywhere = pl.BlockSpec(memory_space=pl.ANY)
    slots, outgoing = pl.pallas_call(
        prepare_kernel,
        out_shape=[jax.ShapeDtypeStruct(shape, BF16) for shape in shapes],
        in_specs=[smem()] + [vmem()] * 2 + [anywhere],
        out_specs=[anywhere] * 2,
        scratch_shapes=[pltpu.VMEM((width, 512), F32)]
        + [pltpu.VMEM(shape, BF16) for shape in shapes]
        + [pltpu.SemaphoreType.DMA((3,))],
        name="prepare",
    )(half, expert_ids.T, tokens, down)
    incoming = lax.ppermute(outgoing, "owner", SWAP_HALF)
    got = lax.all_to_all(
        slots.reshape(EXPERTS, 16, LANES), "shard", split_axis=0, concat_axis=0, tiled=True
    )

    pieces = (8, width // 2, LANES)
    q = pl.pallas_call(
        split_q_kernel,
        out_shape=jax.ShapeDtypeStruct(pieces, BF16),
        in_specs=[vmem()],
        out_specs=vmem(),
        name="splitq",
    )(down)
    q = over_x(q)
    q_keep, q_send = pl.pallas_call(
        turn_q_kernel,
        out_shape=[pltpu.VMEM((32, 8 * width), BF16)] * 2,
        in_specs=[smem(), vmem()],
        out_specs=[vmem()] * 2,
        name="turnq",
    )(half, chip(q))
    q_got = lax.ppermute(q_send, "owner", SWAP_HALF)

    weights = pl.pallas_call(
        load_kernel,
        out_shape=[pltpu.VMEM(gate_weight.shape[1:], BF16)] * 2,
        in_specs=[pl.BlockSpec(memory_space=pl.ANY)] * 2,
        out_specs=[vmem()] * 2,
        scratch_shapes=[pltpu.SemaphoreType.DMA((2,))],
        name="load",
    )(gate_weight[0], up_weight[0])
    keep, send = pl.pallas_call(
        project_kernel,
        out_shape=[jax.ShapeDtypeStruct((NX, 288, LANES), F32), pltpu.VMEM((NX, 288, LANES), F32)],
        in_specs=[smem()] + [vmem()] * 3,
        out_specs=[vmem()] * 2,
        name="project",
    )(core, chip(got.reshape(EXPERTS * 16, LANES)), chip(weights[0]), chip(weights[1]))
    pair = lax.ppermute(send, "owner", SWAP_CORE)
    sums = pl.pallas_call(
        add_kernel,
        out_shape=[pltpu.VMEM(keep.shape[1:], F32)] * NX,
        in_specs=[smem()] + [vmem()] * 2,
        out_specs=[vmem()] * NX,
        name="addcores",
    )(place, keep, chip(pair))
    summed = [sums[0]]
    for d in range(1, NX):
        summed.append(lax.ppermute(sums[d], "owner", ALONG_X[d]))
    mine, theirs = pl.pallas_call(
        fold_kernel,
        out_shape=[pltpu.VMEM((144, LANES), F32)] * 2,
        in_specs=[smem()] + [vmem()] * NX,
        out_specs=[vmem()] * 2,
        name="fold",
    )(half, *[chip(x) for x in summed])

    p = half_of_down(split_p_kernel, pieces, half, down, False, chip(incoming))
    p = over_x(p)

    added = lax.ppermute(theirs, "owner", SWAP_HALF)
    hidden = pl.pallas_call(
        hidden_kernel,
        out_shape=jax.ShapeDtypeStruct((9, FF), BF16),
        in_specs=[vmem()] * 2,
        out_specs=vmem(),
        name="hidden",
    )(chip(mine), chip(added))

    new_down = pl.pallas_call(
        join_kernel,
        out_shape=jax.ShapeDtypeStruct((64, 16 * width), BF16),
        in_specs=[smem()] + [vmem()] * 3,
        out_specs=vmem(),
        name="join",
    )(half, chip(p), chip(q_keep), chip(q_got))
    return hidden.reshape(9, 1, FF), new_down.reshape(1, 64, 16 * width)


def solution(mesh):
    in_specs = (
        P("shard", "owner"),
        P("shard", None),
        P("shard", "owner", None),
        P("shard", "owner", None),
        P("shard", None, "owner"),
    )
    out_specs = (P("owner", "shard", None), P("shard", "owner", None))
    return jax.shard_map(
        on_device, mesh=mesh, in_specs=in_specs, out_specs=out_specs, check_vma=False
    )
```

```python
import jax
import jax.numpy as jnp
from jax import lax
from jax.experimental import pallas as pl
from jax.experimental.pallas import tpu as pltpu
from jax.sharding import PartitionSpec as P


FF = 1024
EXPERTS = 48
NX = 4
LANES = 128
BF16 = jnp.bfloat16
F32 = jnp.float32

OCTET = [list(range(8)), list(range(8, 16))]
ALONG_X = [[(o, o & 9 | (o + 2 * d) & 6) for o in range(16)] for d in range(NX)]
SWAP_CORE = [(o, o ^ 1) for o in range(16)]
SWAP_HALF = [(o, o ^ 8) for o in range(16)]


def iota(shape, dim):
    return lax.broadcasted_iota(jnp.int32, shape, dim)


def vmem():
    return pl.BlockSpec(memory_space=pltpu.VMEM)


def smem():
    return pl.BlockSpec(memory_space=pltpu.SMEM)


def pack_kernel(ids_ref, tokens_ref, out_ref):
    n = EXPERTS * 16
    rows = tokens_ref.shape[0]
    width = tokens_ref.shape[1]
    ids = ids_ref[...]
    line = iota((n, rows), 0)
    expert = line >> 4
    hit = jnp.zeros((n, rows), jnp.bool_)
    for k in range(ids.shape[0]):
        hit = hit | (ids[k : k + 1, :] == expert)
    earlier = jnp.where(iota((rows, rows), 0) < iota((rows, rows), 1), 1.0, 0.0).astype(BF16)
    hits = jnp.where(hit, 1.0, 0.0)
    before = jnp.dot(hits.astype(BF16), earlier, preferred_element_type=F32)
    slot = ((line >> 2) & 3).astype(F32)
    taken = jnp.where(before == slot, hits, 0.0)
    total = jnp.zeros((n, LANES), F32)
    for b in range(4):
        part = tokens_ref[:, b * LANES : min((b + 1) * LANES, width)]
        if part.shape[1] < LANES:
            part = jnp.concatenate([part, jnp.zeros((rows, LANES - part.shape[1]), BF16)], axis=1)
        pick = jnp.where((line & 3) == b, taken, 0.0).astype(BF16)
        total = total + jnp.dot(pick, part, preferred_element_type=F32)
    out_ref[...] = total.astype(BF16)


def project_kernel(core_ref, got_ref, gate_ref, up_ref, keep_ref, send_ref):
    core = core_ref[0]
    n = EXPERTS * 16
    m = 144
    width = gate_ref.shape[0]
    line = iota((m, n), 0)
    other = jnp.where(line >= 72, 1, 0)
    line = line - other * 72
    last = jnp.where(line >= 64, 1, 0)
    xh = jnp.where(last == 1, line - 64, line >> 3)
    s = jnp.where(last == 1, 8, line & 7)
    owner = (xh & 1) * 8 + (xh >> 1) * 2 + (core ^ other)
    slot = owner * 9 + s
    block = (slot * 171) >> 9
    source = block * 16 + (slot - block * 3) * 4
    column = iota((m, n), 1)
    got = got_ref[...]
    parts = []
    for b in range(4):
        pick = jnp.where(column == source + b, 1.0, 0.0).astype(BF16)
        part = jnp.dot(pick, got, preferred_element_type=F32).astype(BF16)
        if (b + 1) * LANES > width:
            part = part[:, : width - b * LANES]
        parts.append(part)
    rows = jnp.concatenate(parts, axis=1)
    gate = jnp.dot(rows, gate_ref[...], preferred_element_type=F32)
    up = jnp.dot(rows, up_ref[...], preferred_element_type=F32)
    for p, out_ref in enumerate((keep_ref, send_ref)):
        for q in range(8):
            x, h = q // 2, q % 2
            for j in range(16):
                src = gate if j < 8 else up
                lane = (j % 8) * LANES
                at = p * 72 + q * 8
                out_ref[x, h * 144 + j * 8 : h * 144 + j * 8 + 8, :] = src[at : at + 8, lane : lane + LANES]
                at = p * 72 + 64 + q
                out_ref[x, h * 144 + 128 + j : h * 144 + 129 + j, :] = src[at : at + 1, lane : lane + LANES]


def hidden_kernel(a_ref, b_ref, out_ref):
    total = a_ref[...] + b_ref[...]

    def gated(v, u):
        return v / (1.0 + jnp.exp(-v)) * u

    tail = gated(total[128:136], total[136:144])
    for j in range(8):
        head = gated(total[j * 8 : j * 8 + 8], total[64 + j * 8 : 72 + j * 8])
        both = jnp.concatenate([head, jnp.broadcast_to(tail[j : j + 1], (8, LANES))], axis=0)
        out_ref[:, j * LANES : (j + 1) * LANES] = both.astype(BF16)[:9]


def add_kernel(x_ref, a_ref, b_ref, *out_refs):
    for d, out_ref in enumerate(out_refs):
        at = (x_ref[0] + d) & 3
        out_ref[...] = a_ref[at] + b_ref[at]


def fold_kernel(half_ref, a_ref, b_ref, c_ref, d_ref, mine_ref, theirs_ref):
    half = half_ref[0]
    for at, out_ref in ((half, mine_ref), (1 - half, theirs_ref)):
        rows = pl.ds(pl.multiple_of(at * 144, 8), 144)
        out_ref[...] = (a_ref[rows] + b_ref[rows]) + (c_ref[rows] + d_ref[rows])


def quarters(parts):
    n = parts[0][0].shape[0]
    group = iota((n, LANES), 1) >> 5
    out = None
    for q, (tile, offset) in enumerate(parts):
        tile = tile.astype(F32)
        if offset != 32 * q:
            tile = pltpu.roll(tile, (32 * q - offset) % LANES, 1)
        out = tile if out is None else jnp.where(group == q, tile, out)
    return out.astype(BF16)


def narrow_kernel(half_ref, down_ref, out_ref):
    for t in range(2):
        parts = []
        for j in range(4 * t, 4 * t + 4):
            k = j // 2 * LANES
            parts.append((down_ref[:, k : k + LANES], j % 2 * 64))
        out_ref[:, t * LANES : (t + 1) * LANES] = quarters(parts)


def split_p_kernel(half_ref, down_ref, got_ref, out_ref):
    n = out_ref.shape[1]
    for j in range(8):
        k, g = j // 2 * LANES, j // 4 * LANES
        parts = []
        for w in range(2):
            rows = slice(w * n, (w + 1) * n)
            parts.append((down_ref[rows, k : k + LANES], j % 2 * 64))
            parts.append((got_ref[rows, g : g + LANES], j % 4 * 32))
        out_ref[j] = quarters(parts)


def split_q_kernel(down_ref, out_ref):
    n = out_ref.shape[1]
    for j in range(8):
        k = j // 2 * LANES
        parts = []
        for w in range(2):
            for h in range(2):
                at = h * 512 + k
                parts.append((down_ref[w * n : (w + 1) * n, at : at + LANES], j % 2 * 64 + 32))
        out_ref[j] = quarters(parts)


def load_kernel(gate_ref, up_ref, gate_out_ref, up_out_ref, sems):
    copies = [
        pltpu.make_async_copy(gate_ref, gate_out_ref, sems.at[0]),
        pltpu.make_async_copy(up_ref, up_out_ref, sems.at[1]),
    ]
    for copy in copies:
        copy.start()
    for copy in copies:
        copy.wait()


def turned(ref):
    n = ref.shape[1]
    low = iota((n, LANES), 1) < 64
    zero = jnp.zeros((n, LANES), BF16)
    parts = []
    for q in range(8):
        block = ref[q]
        parts += [jnp.where(low, block, zero), jnp.where(low, zero, block)]
    stack = jnp.concatenate(parts, axis=0)
    i, k = iota((64, LANES), 0), iota((64, LANES), 1)
    eye = jnp.where((i == k) | (i + 64 == k), 1.0, 0.0).astype(BF16)
    out = lax.dot_general(eye, stack, (((1,), (1,)), ((), ())), preferred_element_type=F32)
    return out.astype(BF16)


def turn_q_kernel(half_ref, in_ref, keep_ref, send_ref):
    rows = turned(in_ref)
    first = half_ref[0] == 0
    keep_ref[...] = jnp.where(first, rows[:32], rows[32:])
    send_ref[...] = jnp.where(first, rows[32:], rows[:32])


def join_kernel(half_ref, p_ref, keep_ref, got_ref, out_ref):
    width = keep_ref.shape[1]
    own = pl.ds(pl.multiple_of(half_ref[0] * width, LANES), width)
    other = pl.ds(pl.multiple_of((1 - half_ref[0]) * width, LANES), width)
    rows = turned(p_ref)
    out_ref[:32, own] = rows[:32]
    out_ref[:32, other] = rows[32:]
    out_ref[32:, own] = keep_ref[...]
    out_ref[32:, other] = got_ref[...]


def chip(x):
    return pltpu.with_memory_space_constraint(x, pltpu.VMEM)


def half_of_down(kernel, out, half, down, other, *more):
    width = down.shape[0]
    return pl.pallas_call(
        kernel,
        out_shape=jax.ShapeDtypeStruct(out, BF16),
        grid_spec=pltpu.PrefetchScalarGridSpec(
            num_scalar_prefetch=1,
            grid=(1,),
            in_specs=[pl.BlockSpec((width, 512), lambda i, h: (0, (1 - h[0]) if other else h[0]))]
            + [vmem() for _ in more],
            out_specs=vmem(),
        ),
    )(half, down, *more)


def over_x(x):
    return lax.all_to_all(
        x, "owner", split_axis=0, concat_axis=0, tiled=True, axis_index_groups=OCTET
    )


def on_device(tokens, expert_ids, gate_weight, up_weight, trainer_down):
    _, width = tokens.shape
    owner = lax.axis_index("owner")
    half = (owner >> 3).astype(jnp.int32).reshape(1)
    core = (owner & 1).astype(jnp.int32).reshape(1)
    place = ((owner >> 1) & 3).astype(jnp.int32).reshape(1)
    down = jnp.swapaxes(trainer_down, 1, 2).reshape(width, 1024)

    outgoing = half_of_down(narrow_kernel, (width, 256), half, down, True)
    incoming = lax.ppermute(outgoing, "owner", SWAP_HALF)

    packed = pl.pallas_call(
        pack_kernel,
        out_shape=jax.ShapeDtypeStruct((EXPERTS * 16, LANES), BF16),
        in_specs=[vmem(), vmem()],
        out_specs=vmem(),
        name="pack",
    )(expert_ids.T, tokens)
    got = lax.all_to_all(
        packed.reshape(EXPERTS, 16, LANES), "shard", split_axis=0, concat_axis=0, tiled=True
    )

    pieces = (8, width // 2, LANES)
    q = pl.pallas_call(
        split_q_kernel,
        out_shape=jax.ShapeDtypeStruct(pieces, BF16),
        in_specs=[vmem()],
        out_specs=vmem(),
        name="splitq",
    )(down)
    q = over_x(q)
    q_keep, q_send = pl.pallas_call(
        turn_q_kernel,
        out_shape=[pltpu.VMEM((32, 8 * width), BF16)] * 2,
        in_specs=[smem(), vmem()],
        out_specs=[vmem()] * 2,
        name="turnq",
    )(half, chip(q))
    q_got = lax.ppermute(q_send, "owner", SWAP_HALF)

    weights = pl.pallas_call(
        load_kernel,
        out_shape=[pltpu.VMEM(gate_weight.shape[1:], BF16)] * 2,
        in_specs=[pl.BlockSpec(memory_space=pl.ANY)] * 2,
        out_specs=[vmem()] * 2,
        scratch_shapes=[pltpu.SemaphoreType.DMA((2,))],
        name="load",
    )(gate_weight[0], up_weight[0])
    keep, send = pl.pallas_call(
        project_kernel,
        out_shape=[jax.ShapeDtypeStruct((NX, 288, LANES), F32), pltpu.VMEM((NX, 288, LANES), F32)],
        in_specs=[smem()] + [vmem()] * 3,
        out_specs=[vmem()] * 2,
        name="project",
    )(core, chip(got.reshape(EXPERTS * 16, LANES)), chip(weights[0]), chip(weights[1]))
    pair = lax.ppermute(send, "owner", SWAP_CORE)
    sums = pl.pallas_call(
        add_kernel,
        out_shape=[pltpu.VMEM(keep.shape[1:], F32)] * NX,
        in_specs=[smem()] + [vmem()] * 2,
        out_specs=[vmem()] * NX,
        name="addcores",
    )(place, keep, chip(pair))
    summed = [sums[0]]
    for d in range(1, NX):
        summed.append(lax.ppermute(sums[d], "owner", ALONG_X[d]))
    mine, theirs = pl.pallas_call(
        fold_kernel,
        out_shape=[pltpu.VMEM((144, LANES), F32)] * 2,
        in_specs=[smem()] + [vmem()] * NX,
        out_specs=[vmem()] * 2,
        name="fold",
    )(half, *[chip(x) for x in summed])

    p = half_of_down(split_p_kernel, pieces, half, down, False, chip(incoming))
    p = over_x(p)

    added = lax.ppermute(theirs, "owner", SWAP_HALF)
    hidden = pl.pallas_call(
        hidden_kernel,
        out_shape=jax.ShapeDtypeStruct((9, FF), BF16),
        in_specs=[vmem()] * 2,
        out_specs=vmem(),
        name="hidden",
    )(chip(mine), chip(added))

    new_down = pl.pallas_call(
        join_kernel,
        out_shape=jax.ShapeDtypeStruct((64, 16 * width), BF16),
        in_specs=[smem()] + [vmem()] * 3,
        out_specs=vmem(),
        name="join",
    )(half, chip(p), chip(q_keep), chip(q_got))
    return hidden.reshape(9, 1, FF), new_down.reshape(1, 64, 16 * width)


def solution(mesh):
    in_specs = (
        P("shard", "owner"),
        P("shard", None),
        P("shard", "owner", None),
        P("shard", "owner", None),
        P("shard", None, "owner"),
    )
    out_specs = (P("owner", "shard", None), P("shard", "owner", None))
    return jax.shard_map(
        on_device, mesh=mesh, in_specs=in_specs, out_specs=out_specs, check_vma=False
    )
```
